32 devices in a mesh: cls: 4 (over y, x), dom: 8 (over z, core).
Axes of the slice: x: 2, y: 2, z: 4, core: 2. Of those that a mesh axis runs over, the one named last changes fastest.
Arguments:
- particles: bfloat16 [256, 2, 110592], P(('cls', 'dom')), may hold values from -18 to 18
- labels: int32 [256, 1], P(('cls', 'dom')), may hold values from 0 to 7; in each aligned block of 8 rows (0 to 7, 8 to 15, ...) at most 2 rows name the same one
- wedge_index: int32 [256], P(('cls', 'dom')), may hold values from 0 to 11
- wedge_table: float32 [12, 110592], replicated, may hold values from 0.05 to 1
Outputs:
- class_average: float32 [8, 2, 110592], P('cls', None, 'dom')
- weight_total: float32 [8, 110592], P('cls', 'dom')
The draws below stay inside these ranges and needn't reach their ends.
Inputs may be any that keep to these rules, and one draw needn't show every extreme that they name: `labels`: among the rows of one device no class appears more than 2 times, and on some devices one class appears exactly 2 times; every class appears on some device.
All inputs are finite; a program needn't handle non-finite values.
Results may differ from the reference program's by a relative error of at most 0.0003.
Values may be sent and summed in bfloat16 or wider, within the bound.
A program may use at most 128 MiB of HBM per device.

```python
import math
import jax
import jax.numpy as jnp
import numpy as np
from jax import lax

P_DEV = 8
WEDGES = 12
CLASSES = 8
MOST = 2
VOX = 110592
PARTICLES = 256


def place_ends(values, stream_key, least, top_value):
    dims = values.shape
    index_at = [jax.random.randint(jax.random.fold_in(stream_key, axis), (), 0, dims[axis]) for axis in range(len(dims))]
    values = values.at[tuple(index_at)].set(least)
    longest = dims.index(max(dims))
    index_at[longest] = (index_at[longest] + 1) % dims[longest]
    return values.at[tuple(index_at)].set(top_value)


def level_of(key, shape, pieces, least, high):
    level = 1.0
    for position, parts in pieces:
        draws = jax.random.uniform(jax.random.fold_in(jax.random.fold_in(key, 6), position), (parts,), jnp.float32, least / len(pieces), high / len(pieces))
        level = level * jnp.repeat(jnp.exp(draws), shape[position] // parts).reshape((-1,) + (1,) * (len(shape) - 1 - position))
    return level


def shared_out(own_key, own, number, rows, count, top, limit, slope):
    ranking = jax.random.permutation(own_key, count)
    heavy_load, ordinary = shares(count, rows * top, limit, slope, True), shares(count, rows * top, limit, slope, False)
    places = jnp.arange(count)

    def named(tallies, turn):
        used = int((tallies > 0).sum())
        fixed = max(1, used // 4)
        shifted = fixed + (places - fixed + turn * (used - fixed)) % max(1, count - fixed)
        return jnp.zeros((count,), jnp.int32).at[ranking[jnp.where(places < fixed, places, shifted)]].set(jnp.asarray(tallies, jnp.int32))

    tallies = jnp.where(number % 4 == 0, named(heavy_load, number // 4), named(ordinary, number - number // 4 - 1))
    mixed = jax.random.permutation(jax.random.fold_in(own, 3), count)
    donor, taker = mixed[0:count // 2 * 2:2], mixed[1:count // 2 * 2:2]
    slack = jnp.minimum(tallies[donor] - 1, limit - tallies[taker]) // 2
    slack = jnp.where((donor == ranking[0]) | (taker == ranking[0]) | (tallies[taker] == 0), 0, jnp.maximum(slack, 0))
    shifted = jax.random.randint(jax.random.fold_in(own, 4), (count // 2,), 0, 1 << 20) % (slack + 1)
    tallies = tallies.at[donor].add(-shifted).at[taker].add(shifted)
    items = jnp.searchsorted(jnp.cumsum(tallies), jnp.arange(rows * top), side="right").astype(jnp.int32)
    grid = items.reshape(top, rows).T
    grid = grid[jax.random.permutation(jax.random.fold_in(own, 1), rows)]
    turn = jax.random.randint(jax.random.fold_in(own, 2), (rows, 1), 0, top)
    return jnp.take_along_axis(grid, (jnp.arange(top)[None, :] + turn) % top, axis=1)


def shares(number_of, total, bound, skew, full):
    loads = [(1 << 20) // math.isqrt(standing ** skew) + 1 for standing in range(1, number_of + 1)]
    largest = bound if full else min(bound, max(-(-total // number_of), total * loads[0] // sum(loads)))
    least = 1 if total - largest >= number_of - 1 else 0
    holding, surplus = [largest] + [least] * (number_of - 1), total - largest - least * (number_of - 1)
    while surplus > 0:
        free = [i for i in range(1, number_of) if holding[i] < largest] or [i for i in range(1, number_of) if holding[i] < bound]
        mass, remaining = sum([loads[i] for i in free]), surplus
        for i in free:
            extra = min(bound - holding[i], max(1, remaining * loads[i] // mass), surplus)
            holding[i] = holding[i] + extra
            surplus = surplus - extra
    return np.array(holding)


def bell_draw(rng, shape, spread, limit, split=(), kind=jnp.bfloat16):
    array = spread * jax.random.normal(rng, shape, jnp.float32)
    if split:
        array = array * level_of(rng, shape, split, -0.22, 0.18)
    return jnp.clip(array, -limit, limit).astype(kind)


def setup_inputs(seed: int = 0) -> dict:
    keys = jax.random.split(jax.random.key(seed), 5)
    particles = bell_draw(keys[0], (PARTICLES, 2, VOX), 3.0, 18.0, ((0, 32),))
    labels_keys = jax.random.split(jax.random.fold_in(keys[1], 1), PARTICLES // P_DEV)
    labels_turns = jax.random.permutation(jax.random.fold_in(keys[1], 3), PARTICLES // P_DEV)
    labels = jax.vmap(lambda own, number: shared_out(jax.random.fold_in(keys[1], 2), own, number, P_DEV, CLASSES, 1, MOST, 2))(labels_keys, labels_turns).reshape((PARTICLES, 1))
    wedge_index = place_ends(jax.random.randint(keys[2], (PARTICLES,), 0, WEDGES), jax.random.fold_in(keys[2], 1), 0, WEDGES - 1).astype(jnp.int32)
    wedge_table = jnp.clip(jnp.exp(jax.random.uniform(keys[3], (WEDGES, VOX), jnp.float32, math.log(0.05), math.log(1.0))), 0.05, 1.0)
    return {"particles": particles, "labels": labels, "wedge_index": wedge_index, "wedge_table": wedge_table}


def reference(particles, labels, wedge_index, wedge_table):
    count = particles.shape[0]
    block = 64 if count % 64 == 0 else count
    steps_total = count // block
    classes_all = CLASSES
    label_flat = labels[:, 0]

    def accumulate(carry, index):
        start = (index * block).astype(jnp.int32)
        piece = lax.dynamic_slice_in_dim(particles, start, block, 0).astype(jnp.float32)
        label_piece = lax.dynamic_slice_in_dim(label_flat, start, block, 0)
        wedge_piece = lax.dynamic_slice_in_dim(wedge_index, start, block, 0)
        pick = (wedge_piece[:, None] == jnp.arange(WEDGES, dtype=jnp.int32)[None, :]).astype(jnp.float32)
        weight = jnp.dot(pick, wedge_table, precision=lax.Precision.HIGHEST)
        member = (jnp.arange(classes_all, dtype=jnp.int32)[:, None] == label_piece[None, :]).astype(jnp.float32)
        numer = jnp.einsum("kb,bcv->kcv", member, weight[:, None, :] * piece, precision=lax.Precision.HIGHEST)
        denom = jnp.dot(member, weight * weight, precision=lax.Precision.HIGHEST)
        return (carry[0] + numer, carry[1] + denom), None

    start_sums = (jnp.zeros((classes_all, 2, VOX), jnp.float32), jnp.zeros((classes_all, VOX), jnp.float32))
    (weighted_sum, weight_total), unused = lax.scan(accumulate, start_sums, jnp.arange(steps_total, dtype=jnp.int32))
    class_average = weighted_sum / (weight_total[:, None, :] + 1.0)
    return class_average, weight_total
```

```python
import functools

import jax
import jax.numpy as jnp
from jax import lax
from jax.experimental import pallas as pl
from jax.experimental.pallas import tpu as pltpu
from jax.sharding import PartitionSpec as P

MESH = pl.DeviceIdType.MESH
LANES = 128
TILE_CAP = 1536
WIRE = jnp.float32


def tile_of(length):
    best = LANES
    for size in range(LANES, TILE_CAP + 1, LANES):
        if length % size == 0:
            best = size
    return best


def split2(value):
    high = value.astype(jnp.bfloat16)
    low = (value - high.astype(jnp.float32)).astype(jnp.bfloat16)
    return high, low


def dot2(left, value):
    high, low = split2(value)
    return jnp.dot(left, high, preferred_element_type=jnp.float32) + jnp.dot(
        left, low, preferred_element_type=jnp.float32
    )


def kernel(
    n_z, shard, rows, group_rows, wedges,
    x_ref, table_ref, aux_ref, avg_ref, total_ref,
    x_own, x_peer, aux_peer, table, sums, r1, mid, r2, last, rz,
    load_sem, pair_send, pair_recv, aux_send, aux_recv,
    s1_send, s1_recv, s2_send, s2_recv, z_send, z_recv,
):
    cls = lax.axis_index("cls")
    dom = lax.axis_index("dom")
    z = dom // 2
    core = lax.rem(dom, 2)
    peer = dom + 1 - 2 * core
    bit0 = lax.rem(cls, 2)
    bit1 = cls // 2
    near = cls + 1 - 2 * bit0
    far = cls + 2 - 4 * bit1
    both = near + 2 - 4 * bit1
    tile = tile_of(shard)

    def place(step):
        return lax.rem(z + 1 + step, n_z)

    loads = []
    for step in range(n_z):
        here = place(step) * 2 + core
        span = pl.ds(pl.multiple_of(here * shard, LANES), shard)
        one = pltpu.make_async_copy(x_ref.at[:, span], x_own.at[step], load_sem.at[step, 0])
        two = pltpu.make_async_copy(table_ref.at[:, span], table.at[step], load_sem.at[step, 1])
        one.start()
        two.start()
        loads.append((one, two))

    barrier = pltpu.get_barrier_semaphore()
    pl.semaphore_signal(barrier, inc=1, device_id={"dom": peer}, device_id_type=MESH)
    pl.semaphore_signal(barrier, inc=1, device_id={"cls": near}, device_id_type=MESH)
    pl.semaphore_signal(barrier, inc=1, device_id={"cls": far}, device_id_type=MESH)
    for step in range(n_z - 1):
        pl.semaphore_signal(
            barrier, inc=1, device_id={"dom": place(step) * 2 + core}, device_id_type=MESH
        )
    pl.semaphore_wait(barrier, n_z + 2)

    aux_copy = pltpu.make_async_remote_copy(
        src_ref=aux_ref, dst_ref=aux_peer, send_sem=aux_send, recv_sem=aux_recv,
        device_id={"dom": peer}, device_id_type=MESH,
    )
    aux_copy.start()
    pair = []
    for step in range(n_z):
        there = place(step) * 2 + (1 - core)
        span = pl.ds(pl.multiple_of(there * shard, LANES), shard)
        copy = pltpu.make_async_remote_copy(
            src_ref=x_ref.at[:, span], dst_ref=x_peer.at[step],
            send_sem=pair_send.at[step], recv_sem=pair_recv.at[step],
            device_id={"dom": peer}, device_id_type=MESH,
        )
        copy.start()
        pair.append(copy)
    aux_copy.wait()

    pick_own = aux_ref[0]
    pick_peer = aux_peer[0]
    pick_own_b = pick_own[:, :wedges].astype(jnp.bfloat16)
    pick_peer_b = pick_peer[:, :wedges].astype(jnp.bfloat16)
    member_own = aux_ref[1][:, :rows].astype(jnp.bfloat16)
    member_peer = aux_peer[1][:, :rows].astype(jnp.bfloat16)
    counts = jnp.dot(
        member_own, pick_own.astype(jnp.bfloat16), preferred_element_type=jnp.float32
    ) + jnp.dot(member_peer, pick_peer.astype(jnp.bfloat16), preferred_element_type=jnp.float32)
    n_groups = sums.shape[1]
    long = shard + LANES

    first, second, third = {}, {}, {}

    def compute(step):
        for copy in loads[step]:
            copy.wait()
        pair[step].wait()
        for group in range(n_groups):
            sums[step, group, :, pl.ds(shard, LANES)] = counts[
                group * group_rows : (group + 1) * group_rows
            ].astype(sums.dtype)

        @pl.loop(0, shard // tile)
        def _(index):
            span = pl.ds(pl.multiple_of(index * tile, LANES), tile)
            high, low = split2(table[step, :, span])
            total = None
            for pick, member, source in (
                (pick_own_b, member_own, x_own),
                (pick_peer_b, member_peer, x_peer),
            ):
                weight = jnp.dot(pick, high, preferred_element_type=jnp.float32) + jnp.dot(
                    pick, low, preferred_element_type=jnp.float32
                )
                part = dot2(member, weight * source[step, :, span].astype(jnp.float32))
                total = part if total is None else total + part
            for group in range(n_groups):
                sums[step, group, :, span] = total[
                    group * group_rows : (group + 1) * group_rows
                ].astype(sums.dtype)

        partner, other = (near, far) if step % 2 == 0 else (far, near)
        copies = []
        for slot, group in ((1, both), (0, partner)):
            copy = pltpu.make_async_remote_copy(
                src_ref=sums.at[step, group], dst_ref=r1.at[step, slot],
                send_sem=s1_send.at[step, slot], recv_sem=s1_recv.at[step, slot],
                device_id={"cls": partner}, device_id_type=MESH,
            )
            copy.start()
            copies.append(copy)
        first[step] = copies

    def forward(step):
        partner, other = (near, far) if step % 2 == 0 else (far, near)
        first[step][0].wait()
        mid[step] = (
            sums[step, other].astype(jnp.float32) + r1[step, 1].astype(jnp.float32)
        ).astype(mid.dtype)
        copy = pltpu.make_async_remote_copy(
            src_ref=mid.at[step], dst_ref=r2.at[step],
            send_sem=s2_send.at[step], recv_sem=s2_recv.at[step],
            device_id={"cls": other}, device_id_type=MESH,
        )
        copy.start()
        second[step] = copy

    def settle(step):
        first[step][1].wait()
        second[step].wait()
        last[step] = (
            sums[step, cls].astype(jnp.float32)
            + r1[step, 0].astype(jnp.float32)
            + r2[step].astype(jnp.float32)
        ).astype(last.dtype)
        if step < n_z - 1:
            copy = pltpu.make_async_remote_copy(
                src_ref=last.at[step], dst_ref=rz.at[step],
                send_sem=z_send.at[step], recv_sem=z_recv.at[step],
                device_id={"dom": place(step) * 2 + core}, device_id_type=MESH,
            )
            copy.start()
            third[step] = copy

    for step in range(n_z):
        compute(step)
        if step >= 2:
            forward(step - 2)
    for step in range(max(n_z - 2, 0), n_z):
        forward(step)
        settle(step - 2) if step >= 2 else None
    for step in range(n_z):
        if step not in third and not (max(n_z - 2, 0) <= step + 2 < n_z):
            settle(step)
    for step in range(n_z - 1):
        third[step].wait()

    tally = last[n_z - 1, :, pl.ds(shard, LANES)].astype(jnp.float32)
    for step in range(n_z - 1):
        tally = tally + rz[step, :, pl.ds(shard, LANES)].astype(jnp.float32)
    tally = tally[:, :wedges]

    @pl.loop(0, shard // tile)
    def _(index):
        span = pl.ds(pl.multiple_of(index * tile, LANES), tile)
        value = last[n_z - 1, :, span].astype(jnp.float32)
        for step in range(n_z - 1):
            value = value + rz[step, :, span].astype(jnp.float32)
        weight = table[n_z - 1, :, span]
        total = jnp.dot(
            tally, weight * weight,
            precision=lax.Precision.HIGHEST, preferred_element_type=jnp.float32,
        )
        mean = value / (total + 1.0)
        for index_k in range(group_rows // 2):
            avg_ref[index_k, :, span] = mean[2 * index_k : 2 * index_k + 2]
            total_ref[pl.ds(index_k, 1), span] = total[2 * index_k : 2 * index_k + 1]


def per_device(classes, particles, labels, wedge_index, wedge_table):
    n_cls = lax.axis_size("cls")
    n_dom = lax.axis_size("dom")
    p_dev, _, voxels = particles.shape
    wedges = wedge_table.shape[0]
    shard = voxels // n_dom
    n_z = n_dom // 2
    group = classes // n_cls
    rows = 2 * p_dev
    all_rows = 2 * classes
    flat = particles.reshape(rows, voxels)
    row = jnp.arange(rows, dtype=jnp.int32)
    lane = jnp.arange(LANES, dtype=jnp.int32)
    out_row = jnp.arange(all_rows, dtype=jnp.int32)
    wedge_row = jnp.repeat(wedge_index, 2)
    label_lane = jnp.pad(jnp.repeat(labels[:, 0], 2), (0, LANES - rows), constant_values=-1)
    pick = (wedge_row[:, None] == lane[None, :]).astype(jnp.float32)
    member = (
        (label_lane[None, :] == out_row[:, None] // 2)
        & (lane[None, :] % 2 == out_row[:, None] % 2)
    ).astype(jnp.float32)
    aux = jnp.stack([pick, member])
    long = shard + LANES
    any_space = pl.BlockSpec(memory_space=pl.ANY)
    vmem = pl.BlockSpec(memory_space=pltpu.VMEM)
    dma = pltpu.SemaphoreType.DMA
    return pl.pallas_call(
        functools.partial(kernel, n_z, shard, rows, 2 * group, wedges),
        out_shape=(
            jax.ShapeDtypeStruct((group, 2, shard), jnp.float32),
            jax.ShapeDtypeStruct((group, shard), jnp.float32),
        ),
        in_specs=[any_space, any_space, vmem],
        out_specs=(vmem, vmem),
        scratch_shapes=[
            pltpu.VMEM((n_z, rows, shard), jnp.bfloat16),
            pltpu.VMEM((n_z, rows, shard), jnp.bfloat16),
            pltpu.VMEM((2, rows, LANES), jnp.float32),
            pltpu.VMEM((n_z, wedges, shard), jnp.float32),
            pltpu.VMEM((n_z, n_cls, 2 * group, long), WIRE),
            pltpu.VMEM((n_z, 2, 2 * group, long), WIRE),
            pltpu.VMEM((n_z, 2 * group, long), WIRE),
            pltpu.VMEM((n_z, 2 * group, long), WIRE),
            pltpu.VMEM((n_z, 2 * group, long), WIRE),
            pltpu.VMEM((n_z, 2 * group, long), WIRE),
            dma((n_z, 2)), dma((n_z,)), dma((n_z,)), dma, dma,
            dma((n_z, 2)), dma((n_z, 2)), dma((n_z,)), dma((n_z,)),
            dma((n_z,)), dma((n_z,)),
        ],
        compiler_params=pltpu.CompilerParams(
            collective_id=0, has_side_effects=True, vmem_limit_bytes=60 * 1024 * 1024
        ),
    )(flat, wedge_table, aux)


CLASSES_PER_GROUP = 2


def solution(mesh):
    classes = CLASSES_PER_GROUP * mesh.shape["cls"]
    return jax.shard_map(
        functools.partial(per_device, classes),
        mesh=mesh,
        in_specs=(P(("cls", "dom"), None, None), P(("cls", "dom"), None), P(("cls", "dom")), P()),
        out_specs=(P("cls", None, "dom"), P("cls", "dom")),
        check_vma=False,
    )
```

```python
import functools

import jax
import jax.numpy as jnp
from jax import lax
from jax.experimental import pallas as pl
from jax.experimental.pallas import tpu as pltpu
from jax.sharding import PartitionSpec as P

MESH = pl.DeviceIdType.MESH
LANES = 128
LEVELS = 32767.0
CLASSES_PER_GROUP = 2


def divisor(number, cap):
    return max(size for size in range(1, cap + 1) if number % size == 0)


def split2(value):
    high = value.astype(jnp.bfloat16)
    low = (value - high.astype(jnp.float32)).astype(jnp.bfloat16)
    return high, low


def dot(left, right):
    return jnp.dot(left, right, preferred_element_type=jnp.float32)


def spans_of(start, tiles, cap):
    unit = divisor(tiles, cap)

    def span(index, base=start):
        return pl.ds(pl.multiple_of(base + index * (unit * LANES), LANES), unit * LANES)

    return tiles // unit, unit, span


def encode(read, tiles, start, code_ref, scale_ref):
    turns, unit, span = spans_of(0, tiles, 9)

    def largest(index, top):
        block = jnp.abs(read(span(index, start)))
        for k in range(unit):
            top = jnp.maximum(top, block[:, k * LANES : (k + 1) * LANES])
        return top

    rows = code_ref.shape[0]
    top = lax.fori_loop(0, turns, largest, jnp.zeros((rows, LANES), jnp.float32))
    top = jnp.maximum(top, 1e-30)
    scale_ref[...] = top * (1.0 / LEVELS)
    factor = jnp.concatenate([LEVELS / top] * unit, axis=1)

    def store(index, carry):
        block = read(span(index, start)) * factor
        code_ref[:, span(index)] = jnp.round(block).astype(jnp.int32).astype(jnp.int16)
        return carry

    lax.fori_loop(0, turns, store, 0)


def decoder(code_ref, scale_ref, start, tiles):
    unit = divisor(tiles, 9)
    scale = jnp.concatenate([scale_ref[...]] * unit, axis=1)

    def read(span):
        here = pl.ds(pl.multiple_of(span.start - start, LANES), span.size)
        return code_ref[:, here].astype(jnp.int32).astype(jnp.float32) * scale

    return read


def kernel(
    n_z, shard, p_dev, group_rows, wedges, cuts,
    labels_ref, wedge_ref, x_ref, table_ref, mean_ref, total_ref,
    x_own, x_peer, aux_own, aux_peer, table, sums, last, tallies,
    load_sem, table_sem, pair_send, pair_recv, aux_send, aux_recv,
    *parts_refs,
):
    cls = lax.axis_index("cls")
    dom = lax.axis_index("dom")
    z = dom // 2
    core = lax.rem(dom, 2)
    peer = dom + 1 - 2 * core
    near = cls + 1 - 2 * lax.rem(cls, 2)
    far = cls + 2 - 4 * (cls // 2)
    both = near + 2 - 4 * (cls // 2)
    n_groups = sums.shape[1]
    rows = 2 * p_dev
    each = len(parts_refs) // len(cuts)
    bufs = [parts_refs[i * each : (i + 1) * each] for i in range(len(cuts))]

    def place(step):
        return lax.rem(z + 1 + step, n_z)

    loads = []
    for step in range(n_z):
        here = place(step) * 2 + core
        span = pl.ds(pl.multiple_of(here * shard, LANES), shard)
        copies = [pltpu.make_async_copy(table_ref.at[:, span], table.at[step], table_sem.at[step])]
        for p in range(p_dev):
            copies.append(
                pltpu.make_async_copy(
                    x_ref.at[p, :, span], x_own.at[step, pl.ds(2 * p, 2)], load_sem.at[step, p]
                )
            )
        for copy in copies:
            copy.start()
        loads.append(copies)

    barrier = pltpu.get_barrier_semaphore()
    pl.semaphore_signal(barrier, inc=1, device_id={"dom": peer}, device_id_type=MESH)
    pl.semaphore_signal(barrier, inc=1, device_id={"cls": near}, device_id_type=MESH)
    pl.semaphore_signal(barrier, inc=1, device_id={"cls": far}, device_id_type=MESH)
    for step in range(n_z - 1):
        pl.semaphore_signal(
            barrier, inc=1, device_id={"dom": place(step) * 2 + core}, device_id_type=MESH
        )

    row = lax.broadcasted_iota(jnp.int32, (rows, LANES), 0)
    lane = lax.broadcasted_iota(jnp.int32, (rows, LANES), 1)
    out_row = lax.broadcasted_iota(jnp.int32, (n_groups * group_rows, LANES), 0)
    out_lane = lax.broadcasted_iota(jnp.int32, (n_groups * group_rows, LANES), 1)
    wedge_of = jnp.zeros((rows, LANES), jnp.int32)
    label_of = jnp.zeros_like(out_row) - 1
    for p in range(p_dev):
        wedge_of = jnp.where((row == 2 * p) | (row == 2 * p + 1), wedge_ref[p], wedge_of)
        label_of = jnp.where(
            (out_lane == 2 * p) | (out_lane == 2 * p + 1), labels_ref[p], label_of
        )
    aux_own[0] = (wedge_of == lane).astype(jnp.float32)
    aux_own[1] = (
        (out_row == 2 * label_of + (out_lane & 1)) & (label_of >= 0)
    ).astype(jnp.float32)

    pl.semaphore_wait(barrier, n_z + 2)

    pair = []
    for step in range(n_z):
        there = place(step) * 2 + (1 - core)
        span = pl.ds(pl.multiple_of(there * shard, LANES), shard)
        copies = []
        for p in range(p_dev):
            copy = pltpu.make_async_remote_copy(
                src_ref=x_ref.at[p, :, span], dst_ref=x_peer.at[step, pl.ds(2 * p, 2)],
                send_sem=pair_send.at[step, p], recv_sem=pair_recv.at[step, p],
                device_id={"dom": peer}, device_id_type=MESH,
            )
            copy.start()
            copies.append(copy)
        pair.append(copies)
    aux_copy = pltpu.make_async_remote_copy(
        src_ref=aux_own, dst_ref=aux_peer, send_sem=aux_send, recv_sem=aux_recv,
        device_id={"dom": peer}, device_id_type=MESH,
    )
    aux_copy.start()
    aux_copy.wait()

    pick_own = aux_own[0].astype(jnp.bfloat16)
    pick_peer = aux_peer[0].astype(jnp.bfloat16)
    member_own = aux_own[1][:, :rows].astype(jnp.bfloat16)
    member_peer = aux_peer[1][:, :rows].astype(jnp.bfloat16)
    counts = dot(member_own, pick_own) + dot(member_peer, pick_peer)
    for group in range(n_groups):
        tallies[group] = counts[group * group_rows : (group + 1) * group_rows]
    pick_own = pick_own[:, :wedges]
    pick_peer = pick_peer[:, :wedges]

    def send(source, target, sems, slot, who):
        copy = pltpu.make_async_remote_copy(
            src_ref=source, dst_ref=target, send_sem=sems[0].at[slot], recv_sem=sems[1].at[slot],
            device_id=who, device_id_type=MESH,
        )
        copy.start()
        return copy

    first, second, third = {}, {}, {}

    def compute(step, part):
        start, tiles = cuts[part]
        (q1, c1, r1, d1, q2, c2, r2, d2, q3, c3, r3, d3, sa, sb, ra, rb) = bufs[part]
        if part == 0:
            for copy in loads[step] + pair[step]:
                copy.wait()
        turns, unit, span_of = spans_of(start, tiles, 12)

        @pl.loop(0, turns)
        def _(index):
            span = span_of(index)
            high, low = split2(table[step, :, span])
            total = None
            for pick, member, source in (
                (pick_own, member_own, x_own),
                (pick_peer, member_peer, x_peer),
            ):
                weight = dot(pick, high) + dot(pick, low)
                up, down = split2(weight * source[step, :, span].astype(jnp.float32))
                piece = dot(member, up) + dot(member, down)
                total = piece if total is None else total + piece
            for group in range(n_groups):
                sums[step, group, :, span] = total[group * group_rows : (group + 1) * group_rows]

        partner = near if part == 0 else far
        copies = []
        for slot, group in ((1, both), (0, partner)):
            encode(
                lambda span: sums[step, group, :, span], tiles, start,
                q1.at[step, slot], c1.at[step, slot, :, pl.ds(0, LANES)],
            )
            if part == 0:
                c1[step, slot, :, pl.ds(LANES, LANES)] = tallies[group]
            for kind, source, target in ((0, c1, d1), (1, q1, r1)):
                copies.append(
                    send(
                        source.at[step, slot], target.at[step, slot], (sa, ra),
                        4 * step + 2 * slot + kind, {"cls": partner},
                    )
                )
        first[step, part] = copies

    def forward(step, part):
        start, tiles = cuts[part]
        (q1, c1, r1, d1, q2, c2, r2, d2, q3, c3, r3, d3, sa, sb, ra, rb) = bufs[part]
        other = far if part == 0 else near
        for copy in first[step, part][:2]:
            copy.wait()
        got = decoder(r1.at[step, 1], d1.at[step, 1, :, pl.ds(0, LANES)], start, tiles)
        encode(
            lambda span: sums[step, other, :, span] + got(span), tiles, start,
            q2.at[step], c2.at[step, :, pl.ds(0, LANES)],
        )
        if part == 0:
            c2[step, :, pl.ds(LANES, LANES)] = tallies[other] + d1[step, 1, :, pl.ds(LANES, LANES)]
        second[step, part] = [
            send(source.at[step], target.at[step], (sb, rb), 4 * step + kind, {"cls": other})
            for kind, source, target in ((0, c2, d2), (1, q2, r2))
        ]

    def settle(step, part):
        start, tiles = cuts[part]
        (q1, c1, r1, d1, q2, c2, r2, d2, q3, c3, r3, d3, sa, sb, ra, rb) = bufs[part]
        for copy in first[step, part][2:] + second[step, part]:
            copy.wait()
        got1 = decoder(r1.at[step, 0], d1.at[step, 0, :, pl.ds(0, LANES)], start, tiles)
        got2 = decoder(r2.at[step], d2.at[step, :, pl.ds(0, LANES)], start, tiles)

        def read(span):
            return sums[step, cls, :, span] + got1(span) + got2(span)

        tally = None
        if part == 0:
            tally = (
                tallies[cls]
                + d1[step, 0, :, pl.ds(LANES, LANES)]
                + d2[step, :, pl.ds(LANES, LANES)]
            )
        if step == n_z - 1:
            turns, _, span_of = spans_of(start, tiles, 9)

            @pl.loop(0, turns)
            def _(index):
                span = span_of(index)
                last[:, span] = read(span)

            return tally
        encode(read, tiles, start, q3.at[step], c3.at[step, :, pl.ds(0, LANES)])
        if part == 0:
            c3[step, :, pl.ds(LANES, LANES)] = tally
        there = place(step) * 2 + core
        third[step, part] = [
            send(source.at[step], target.at[step], (sb, rb), 4 * step + 2 + kind, {"dom": there})
            for kind, source, target in ((0, c3, d3), (1, q3, r3))
        ]
        return None

    n_parts = len(cuts)
    units = [(step, part) for step in range(n_z) for part in range(n_parts)]
    tally = None
    for turn in range(len(units) + 4):
        if turn < len(units):
            compute(*units[turn])
        if 2 <= turn < len(units) + 2:
            forward(*units[turn - 2])
        if 4 <= turn:
            found = settle(*units[turn - 4])
            tally = found if found is not None else tally

    for part in range(n_parts):
        start, tiles = cuts[part]
        (q1, c1, r1, d1, q2, c2, r2, d2, q3, c3, r3, d3, sa, sb, ra, rb) = bufs[part]
        for step in range(n_z - 1):
            for copy in third[step, part]:
                copy.wait()
        if part == 0:
            for step in range(n_z - 1):
                tally = tally + d3[step, :, pl.ds(LANES, LANES)]
            tally = tally[:, :wedges]
        got = [
            decoder(r3.at[step], d3.at[step, :, pl.ds(0, LANES)], start, tiles)
            for step in range(n_z - 1)
        ]
        turns, _, span_of = spans_of(start, tiles, 9)

        @pl.loop(0, turns)
        def _(index):
            span = span_of(index)
            value = last[:, span]
            for read in got:
                value = value + read(span)
            weight = table[n_z - 1, :, span]
            total = jnp.dot(
                tally, weight * weight,
                precision=lax.Precision.HIGHEST, preferred_element_type=jnp.float32,
            )
            mean_ref[:, span] = value / (total + 1.0)
            total_ref[:, span] = total


def finish(mean_ref, total_ref, avg_out, total_out):
    for index in range(avg_out.shape[0]):
        avg_out[index] = mean_ref[pl.ds(2 * index, 2)]
        total_out[pl.ds(index, 1)] = total_ref[pl.ds(2 * index, 1)]


def per_device(classes, particles, labels, wedge_index, wedge_table):
    n_cls = lax.axis_size("cls")
    n_dom = lax.axis_size("dom")
    p_dev, _, voxels = particles.shape
    wedges = wedge_table.shape[0]
    shard = voxels // n_dom
    n_z = n_dom // 2
    group = classes // n_cls
    rows = 2 * p_dev
    out_rows = 2 * group
    tiles = shard // LANES
    cuts = ((0, tiles // 2), (tiles // 2 * LANES, tiles - tiles // 2))
    any_space = pl.BlockSpec(memory_space=pl.ANY)
    vmem = pl.BlockSpec(memory_space=pltpu.VMEM)
    smem = pl.BlockSpec(memory_space=pltpu.SMEM)
    dma = pltpu.SemaphoreType.DMA
    scratch = [
        pltpu.VMEM((n_z, rows, shard), jnp.bfloat16),
        pltpu.VMEM((n_z, rows, shard), jnp.bfloat16),
        pltpu.VMEM((2, rows, LANES), jnp.float32),
        pltpu.VMEM((2, rows, LANES), jnp.float32),
        pltpu.VMEM((n_z, wedges, shard), jnp.float32),
        pltpu.VMEM((n_z, n_cls, out_rows, shard), jnp.float32),
        pltpu.VMEM((out_rows, shard), jnp.float32),
        pltpu.VMEM((n_cls, out_rows, LANES), jnp.float32),
        dma((n_z, p_dev)), dma((n_z,)), dma((n_z, p_dev)), dma((n_z, p_dev)), dma, dma,
    ]
    for part, (_, count) in enumerate(cuts):
        wide = LANES * (2 if part == 0 else 1)
        for lead in ((n_z, 2), (n_z,), (n_z,)):
            for _ in range(2):
                scratch.append(pltpu.VMEM((*lead, out_rows, count * LANES), jnp.int16))
                scratch.append(pltpu.VMEM((*lead, out_rows, wide), jnp.float32))
        scratch += [dma((4 * n_z,)) for _ in range(4)]
    mean, total = pl.pallas_call(
        functools.partial(kernel, n_z, shard, p_dev, out_rows, wedges, cuts),
        out_shape=(
            jax.ShapeDtypeStruct((out_rows, shard), jnp.float32),
            jax.ShapeDtypeStruct((out_rows, shard), jnp.float32),
        ),
        in_specs=[smem, smem, any_space, any_space],
        out_specs=(vmem, vmem),
        scratch_shapes=scratch,
        compiler_params=pltpu.CompilerParams(
            collective_id=0, has_side_effects=True, vmem_limit_bytes=60 * 1024 * 1024
        ),
    )(labels.reshape(p_dev), wedge_index, particles, wedge_table)
    return pl.pallas_call(
        finish,
        out_shape=(
            jax.ShapeDtypeStruct((group, 2, shard), jnp.float32),
            jax.ShapeDtypeStruct((group, shard), jnp.float32),
        ),
        in_specs=[vmem, vmem],
        out_specs=(vmem, vmem),
    )(mean, total)


def solution(mesh):
    classes = CLASSES_PER_GROUP * mesh.shape["cls"]
    return jax.shard_map(
        functools.partial(per_device, classes),
        mesh=mesh,
        in_specs=(P(("cls", "dom"), None, None), P(("cls", "dom"), None), P(("cls", "dom")), P()),
        out_specs=(P("cls", None, "dom"), P("cls", "dom")),
        check_vma=False,
    )
```

```python
import functools

import jax
import jax.numpy as jnp
from jax import lax
from jax.experimental import pallas as pl
from jax.experimental.pallas import tpu as pltpu
from jax.sharding import PartitionSpec as P

MESH = pl.DeviceIdType.MESH
LANES = 128
LEVELS = 32767.0
CLASSES_PER_GROUP = 2


def divisor(number, cap):
    return max(size for size in range(1, cap + 1) if number % size == 0)


def split2(value):
    high = value.astype(jnp.bfloat16)
    low = (value - high.astype(jnp.float32)).astype(jnp.bfloat16)
    return high, low


def stack2(value):
    high = value.astype(jnp.bfloat16).astype(jnp.float32)
    return jnp.concatenate([high, value - high], axis=0).astype(jnp.bfloat16)


def dot(left, right):
    return jnp.dot(left, right, preferred_element_type=jnp.float32)


def spans_of(start, tiles, cap):
    unit = divisor(tiles, cap)

    def span(index, base=start):
        return pl.ds(pl.multiple_of(base + index * (unit * LANES), LANES), unit * LANES)

    return tiles // unit, unit, span


def encode(read, tiles, start, code_ref, scale_ref):
    turns, unit, span = spans_of(0, tiles, 9)

    def largest(index, top):
        block = jnp.abs(read(span(index, start)))
        for k in range(unit):
            top = jnp.maximum(top, block[:, k * LANES : (k + 1) * LANES])
        return top

    rows = code_ref.shape[0]
    top = lax.fori_loop(0, turns, largest, jnp.zeros((rows, LANES), jnp.float32))
    top = jnp.maximum(top, 1e-30)
    scale_ref[...] = top * (1.0 / LEVELS)
    factor = jnp.concatenate([LEVELS / top] * unit, axis=1)

    def store(index, carry):
        block = read(span(index, start)) * factor
        code_ref[:, span(index)] = jnp.round(block).astype(jnp.int32).astype(jnp.int16)
        return carry

    lax.fori_loop(0, turns, store, 0)


def decoder(code_ref, scale_ref, start, tiles):
    unit = divisor(tiles, 9)
    scale = jnp.concatenate([scale_ref[...]] * unit, axis=1)

    def read(span):
        here = pl.ds(pl.multiple_of(span.start - start, LANES), span.size)
        return code_ref[:, here].astype(jnp.int32).astype(jnp.float32) * scale

    return read


def kernel(
    n_z, shard, p_dev, group_rows, wedges, cuts,
    labels_ref, wedge_ref, x_ref, table_ref, mean_ref, total_ref,
    x_all, aux_own, aux_peer, table, sums, last, tallies,
    load_sem, table_sem, pair_send, pair_recv, aux_send, aux_recv,
    *parts_refs,
):
    cls = lax.axis_index("cls")
    dom = lax.axis_index("dom")
    z = dom // 2
    core = lax.rem(dom, 2)
    peer = dom + 1 - 2 * core
    near = cls + 1 - 2 * lax.rem(cls, 2)
    far = cls + 2 - 4 * (cls // 2)
    both = near + 2 - 4 * (cls // 2)
    n_groups = sums.shape[1]
    rows = 2 * p_dev
    each = len(parts_refs) // len(cuts)
    bufs = [parts_refs[i * each : (i + 1) * each] for i in range(len(cuts))]

    def place(step):
        return lax.rem(z + 1 + step, n_z)

    loads = []
    for step in range(n_z):
        here = place(step) * 2 + core
        span = pl.ds(pl.multiple_of(here * shard, LANES), shard)
        copies = [pltpu.make_async_copy(table_ref.at[:, span], table.at[step], table_sem.at[step])]
        for p in range(p_dev):
            copies.append(
                pltpu.make_async_copy(
                    x_ref.at[p, :, span], x_all.at[step, pl.ds(2 * p, 2)], load_sem.at[step, p]
                )
            )
        for copy in copies:
            copy.start()
        loads.append(copies)

    barrier = pltpu.get_barrier_semaphore()
    pl.semaphore_signal(barrier, inc=1, device_id={"dom": peer}, device_id_type=MESH)
    pl.semaphore_signal(barrier, inc=1, device_id={"cls": near}, device_id_type=MESH)
    pl.semaphore_signal(barrier, inc=1, device_id={"cls": far}, device_id_type=MESH)
    for step in range(n_z - 1):
        pl.semaphore_signal(
            barrier, inc=1, device_id={"dom": place(step) * 2 + core}, device_id_type=MESH
        )

    row = lax.broadcasted_iota(jnp.int32, (rows, LANES), 0)
    lane = lax.broadcasted_iota(jnp.int32, (rows, LANES), 1)
    out_row = lax.broadcasted_iota(jnp.int32, (n_groups * group_rows, LANES), 0)
    out_lane = lax.broadcasted_iota(jnp.int32, (n_groups * group_rows, LANES), 1)
    wedge_of = jnp.zeros((rows, LANES), jnp.int32)
    label_of = jnp.zeros_like(out_row) - 1
    for p in range(p_dev):
        wedge_of = jnp.where((row == 2 * p) | (row == 2 * p + 1), wedge_ref[p], wedge_of)
        label_of = jnp.where(
            (out_lane == 2 * p) | (out_lane == 2 * p + 1), labels_ref[p], label_of
        )
    aux_own[0] = (wedge_of == lane).astype(jnp.float32)
    aux_own[1] = (
        (out_row == 2 * label_of + (out_lane & 1)) & (label_of >= 0)
    ).astype(jnp.float32)

    pl.semaphore_wait(barrier, n_z + 2)

    pair = []
    for step in range(n_z):
        there = place(step) * 2 + (1 - core)
        span = pl.ds(pl.multiple_of(there * shard, LANES), shard)
        copies = []
        for p in range(p_dev):
            copy = pltpu.make_async_remote_copy(
                src_ref=x_ref.at[p, :, span], dst_ref=x_all.at[step, pl.ds(rows + 2 * p, 2)],
                send_sem=pair_send.at[step, p], recv_sem=pair_recv.at[step, p],
                device_id={"dom": peer}, device_id_type=MESH,
            )
            copy.start()
            copies.append(copy)
        pair.append(copies)
    aux_copy = pltpu.make_async_remote_copy(
        src_ref=aux_own, dst_ref=aux_peer, send_sem=aux_send, recv_sem=aux_recv,
        device_id={"dom": peer}, device_id_type=MESH,
    )
    aux_copy.start()
    aux_copy.wait()

    pick_own = aux_own[0].astype(jnp.bfloat16)
    pick_peer = aux_peer[0].astype(jnp.bfloat16)
    member_own = aux_own[1][:, :rows].astype(jnp.bfloat16)
    member_peer = aux_peer[1][:, :rows].astype(jnp.bfloat16)
    counts = dot(member_own, pick_own) + dot(member_peer, pick_peer)
    for group in range(n_groups):
        tallies[group] = counts[group * group_rows : (group + 1) * group_rows]
    pick = jnp.concatenate([aux_own[0], aux_peer[0]], axis=0)[:, :wedges]
    pick = jnp.concatenate([pick, pick], axis=1).astype(jnp.bfloat16)
    member = jnp.concatenate([aux_own[1][:, :rows], aux_peer[1][:, :rows]] * 2, axis=1)
    member = member.astype(jnp.bfloat16)

    def send(source, target, sems, slot, who):
        copy = pltpu.make_async_remote_copy(
            src_ref=source, dst_ref=target, send_sem=sems[0].at[slot], recv_sem=sems[1].at[slot],
            device_id=who, device_id_type=MESH,
        )
        copy.start()
        return copy

    first, second, third = {}, {}, {}

    def compute(step, part):
        start, tiles = cuts[part]
        (q1, c1, r1, d1, q2, c2, r2, d2, q3, c3, r3, d3, sa, sb, ra, rb) = bufs[part]
        if part == 0:
            for copy in loads[step] + pair[step]:
                copy.wait()
        turns, unit, span_of = spans_of(start, tiles, 12)

        @pl.loop(0, turns)
        def _(index):
            span = span_of(index)
            weight = dot(pick, stack2(table[step, :, span]))
            high, low = split2(weight * x_all[step, :, span].astype(jnp.float32))
            total = dot(member, jnp.concatenate([high, low], axis=0))
            for group in range(n_groups):
                sums[step, group, :, span] = total[group * group_rows : (group + 1) * group_rows]

        partner = near if part == 0 else far
        copies = []
        for slot, group in ((1, both), (0, partner)):
            encode(
                lambda span: sums[step, group, :, span], tiles, start,
                q1.at[step, slot], c1.at[step, slot, :, pl.ds(0, LANES)],
            )
            if part == 0:
                c1[step, slot, :, pl.ds(LANES, LANES)] = tallies[group]
            for kind, source, target in ((0, c1, d1), (1, q1, r1)):
                copies.append(
                    send(
                        source.at[step, slot], target.at[step, slot], (sa, ra),
                        4 * step + 2 * slot + kind, {"cls": partner},
                    )
                )
        first[step, part] = copies

    def forward(step, part):
        start, tiles = cuts[part]
        (q1, c1, r1, d1, q2, c2, r2, d2, q3, c3, r3, d3, sa, sb, ra, rb) = bufs[part]
        other = far if part == 0 else near
        for copy in first[step, part][:2]:
            copy.wait()
        got = decoder(r1.at[step, 1], d1.at[step, 1, :, pl.ds(0, LANES)], start, tiles)
        encode(
            lambda span: sums[step, other, :, span] + got(span), tiles, start,
            q2.at[step], c2.at[step, :, pl.ds(0, LANES)],
        )
        if part == 0:
            c2[step, :, pl.ds(LANES, LANES)] = tallies[other] + d1[step, 1, :, pl.ds(LANES, LANES)]
        second[step, part] = [
            send(source.at[step], target.at[step], (sb, rb), 4 * step + kind, {"cls": other})
            for kind, source, target in ((0, c2, d2), (1, q2, r2))
        ]

    def settle(step, part):
        start, tiles = cuts[part]
        (q1, c1, r1, d1, q2, c2, r2, d2, q3, c3, r3, d3, sa, sb, ra, rb) = bufs[part]
        for copy in first[step, part][2:] + second[step, part]:
            copy.wait()
        got1 = decoder(r1.at[step, 0], d1.at[step, 0, :, pl.ds(0, LANES)], start, tiles)
        got2 = decoder(r2.at[step], d2.at[step, :, pl.ds(0, LANES)], start, tiles)

        def read(span):
            return sums[step, cls, :, span] + got1(span) + got2(span)

        tally = None
        if part == 0:
            tally = (
                tallies[cls]
                + d1[step, 0, :, pl.ds(LANES, LANES)]
                + d2[step, :, pl.ds(LANES, LANES)]
            )
        if step == n_z - 1:
            turns, _, span_of = spans_of(start, tiles, 9)

            @pl.loop(0, turns)
            def _(index):
                span = span_of(index)
                last[:, span] = read(span)

            return tally
        encode(read, tiles, start, q3.at[step], c3.at[step, :, pl.ds(0, LANES)])
        if part == 0:
            c3[step, :, pl.ds(LANES, LANES)] = tally
        there = place(step) * 2 + core
        third[step, part] = [
            send(source.at[step], target.at[step], (sb, rb), 4 * step + 2 + kind, {"dom": there})
            for kind, source, target in ((0, c3, d3), (1, q3, r3))
        ]
        return None

    n_parts = len(cuts)
    units = [(step, part) for step in range(n_z) for part in range(n_parts)]
    tally = None
    for turn in range(len(units) + 4):
        if turn < len(units):
            compute(*units[turn])
        if 2 <= turn < len(units) + 2:
            forward(*units[turn - 2])
        if 4 <= turn:
            found = settle(*units[turn - 4])
            tally = found if found is not None else tally

    for part in range(n_parts):
        start, tiles = cuts[part]
        (q1, c1, r1, d1, q2, c2, r2, d2, q3, c3, r3, d3, sa, sb, ra, rb) = bufs[part]
        for step in range(n_z - 1):
            for copy in third[step, part]:
                copy.wait()
        if part == 0:
            for step in range(n_z - 1):
                tally = tally + d3[step, :, pl.ds(LANES, LANES)]
            tally = stack2(tally[:, :wedges])
            tally = jnp.concatenate([tally, tally], axis=1)
        got = [
            decoder(r3.at[step], d3.at[step, :, pl.ds(0, LANES)], start, tiles)
            for step in range(n_z - 1)
        ]
        turns, _, span_of = spans_of(start, tiles, 9)

        @pl.loop(0, turns)
        def _(index):
            span = span_of(index)
            value = last[:, span]
            for read in got:
                value = value + read(span)
            weight = table[n_z - 1, :, span]
            total = dot(tally, stack2(weight * weight))
            total = total[:group_rows] + total[group_rows:]
            mean_ref[:, span] = value / (total + 1.0)
            total_ref[:, span] = total


def finish(mean_ref, total_ref, avg_out, total_out):
    for index in range(avg_out.shape[0]):
        avg_out[index] = mean_ref[pl.ds(2 * index, 2)]
        total_out[pl.ds(index, 1)] = total_ref[pl.ds(2 * index, 1)]


def per_device(classes, particles, labels, wedge_index, wedge_table):
    n_cls = lax.axis_size("cls")
    n_dom = lax.axis_size("dom")
    p_dev, _, voxels = particles.shape
    wedges = wedge_table.shape[0]
    shard = voxels // n_dom
    n_z = n_dom // 2
    group = classes // n_cls
    rows = 2 * p_dev
    out_rows = 2 * group
    tiles = shard // LANES
    cuts = ((0, tiles // 2), (tiles // 2 * LANES, tiles - tiles // 2))
    any_space = pl.BlockSpec(memory_space=pl.ANY)
    vmem = pl.BlockSpec(memory_space=pltpu.VMEM)
    smem = pl.BlockSpec(memory_space=pltpu.SMEM)
    dma = pltpu.SemaphoreType.DMA
    scratch = [
        pltpu.VMEM((n_z, 2 * rows, shard), jnp.bfloat16),
        pltpu.VMEM((2, rows, LANES), jnp.float32),
        pltpu.VMEM((2, rows, LANES), jnp.float32),
        pltpu.VMEM((n_z, wedges, shard), jnp.float32),
        pltpu.VMEM((n_z, n_cls, out_rows, shard), jnp.float32),
        pltpu.VMEM((out_rows, shard), jnp.float32),
        pltpu.VMEM((n_cls, out_rows, LANES), jnp.float32),
        dma((n_z, p_dev)), dma((n_z,)), dma((n_z, p_dev)), dma((n_z, p_dev)), dma, dma,
    ]
    for part, (_, count) in enumerate(cuts):
        wide = LANES * (2 if part == 0 else 1)
        for lead in ((n_z, 2), (n_z,), (n_z,)):
            for _ in range(2):
                scratch.append(pltpu.VMEM((*lead, out_rows, count * LANES), jnp.int16))
                scratch.append(pltpu.VMEM((*lead, out_rows, wide), jnp.float32))
        scratch += [dma((4 * n_z,)) for _ in range(4)]
    mean, total = pl.pallas_call(
        functools.partial(kernel, n_z, shard, p_dev, out_rows, wedges, cuts),
        out_shape=(
            jax.ShapeDtypeStruct((out_rows, shard), jnp.float32),
            jax.ShapeDtypeStruct((out_rows, shard), jnp.float32),
        ),
        in_specs=[smem, smem, any_space, any_space],
        out_specs=(vmem, vmem),
        scratch_shapes=scratch,
        compiler_params=pltpu.CompilerParams(
            collective_id=0, has_side_effects=True, vmem_limit_bytes=60 * 1024 * 1024
        ),
    )(labels.reshape(p_dev), wedge_index, particles, wedge_table)
    return pl.pallas_call(
        finish,
        out_shape=(
            jax.ShapeDtypeStruct((group, 2, shard), jnp.float32),
            jax.ShapeDtypeStruct((group, shard), jnp.float32),
        ),
        in_specs=[vmem, vmem],
        out_specs=(vmem, vmem),
    )(mean, total)


def solution(mesh):
    classes = CLASSES_PER_GROUP * mesh.shape["cls"]
    return jax.shard_map(
        functools.partial(per_device, classes),
        mesh=mesh,
        in_specs=(P(("cls", "dom"), None, None), P(("cls", "dom"), None), P(("cls", "dom")), P()),
        out_specs=(P("cls", None, "dom"), P("cls", "dom")),
        check_vma=False,
    )
```
